32 devices in a mesh: ga: 2 (over y), gx: 4 (over z), gy: 2 (over x), gz: 2 (over core).
Axes of the slice: x: 2, y: 2, z: 4, core: 2. Of those that a mesh axis runs over, the one named last changes fastest.
Arguments:
- state: bfloat16 [8, 256, 4, 512], P(('ga', 'gx'), None, None, 'gy'), parts along dimension 0, may hold values from -6 to 6
- left_env: bfloat16 [16, 8, 256, 256], P(None, ('ga', 'gx')), parts along dimension 1, may hold values from -0.375 to 0.375
- mpo_terms: bfloat16 [16, 16, 4, 4], P(None, 'gz'), may hold values from -0.75 to 0.75
- right_env: bfloat16 [16, 1024, 256], P('gz', ('ga', 'gy')), parts along dimension 1, may hold values from -0.09375 to 0.09375
- term_charge: int32 [16], replicated, may hold values from 0 to 2, as said below
- charge_order: int32 [8], P('ga'), parts along dimension 0, may hold values from 0 to 3, as said below
- sector_dims: int32 [8], P('ga'), parts along dimension 0, may hold values from 128 to 256
Outputs:
- result_state: bfloat16 [8, 256, 4, 512], P(('ga', 'gx'), None, 'gz', 'gy'), parts along dimension 0
The draws below stay inside these ranges and needn't reach their ends.
There are 2 independent parts, one for each index of `ga`. The reference program is written for one: setup_inputs(seed, part) draws one part's arguments, and reference() takes and returns one part's arrays. A program takes and returns all parts, laid end to end along the dimension named above; an argument that names none is the same for every part. Nothing has to cross between parts.
Inputs may be any that keep to these rules, and one draw needn't show every extreme that they name: `charge_order`: each value appears once. `term_charge`: each of 0, 1 and 2 appears at least once.
All inputs are finite; a program needn't handle non-finite values.
Results may differ from the reference program's by a relative error of at most 0.0057.
Values may be sent and summed in bfloat16 or wider, within the bound.
A program may use at most 64 MiB of HBM per device.

```python
import jax
import jax.numpy as jnp
from jax import lax

BLK = 256
P_SIZE = 4
RB = 256
W = 16
NS = 4
NR = 512


def draw_charge_order(key, part):
    half_count = NS // 2
    order_key = jax.random.fold_in(key, 11)
    flip_key = jax.random.fold_in(key, 12)
    pair_ids = jax.random.permutation(order_key, half_count).astype(jnp.int32)
    flips = jax.random.randint(flip_key, (half_count,), 0, 2).astype(jnp.int32)
    lower = 2 * pair_ids + flips
    upper = 2 * pair_ids + 1 - flips
    return jnp.concatenate([lower, upper]).astype(jnp.int32)


def draw_term_charge(key, part):
    base_key = jax.random.fold_in(key, 21)
    place_key = jax.random.fold_in(key, 22)
    base = jax.random.randint(base_key, (W,), 0, 3).astype(jnp.int32)
    placing = jax.random.permutation(place_key, W).astype(jnp.int32)
    inverse = jnp.argsort(placing).astype(jnp.int32)
    return jnp.where(inverse < 3, inverse, base).astype(jnp.int32)


def with_ends(result, stream_key, low, top_value):
    longest = result.shape.index(max(result.shape))
    spots = []
    for shift in (0, 1):
        where = [jax.random.randint(jax.random.fold_in(stream_key, axis), (), 0, length) for axis, length in enumerate(result.shape)]
        where[longest] = (where[longest] + shift) % result.shape[longest]
        spots.append(tuple(where))
    return result.at[spots[0]].set(low).at[spots[1]].set(top_value)


def shard_levels(key, extent, split, low, top_value):
    loudness, own = 1.0, jax.random.fold_in(key, 6)
    for dim, shards_of in split:
        draws = jnp.exp(jax.random.uniform(jax.random.fold_in(own, dim), (shards_of,), jnp.float32, low / len(split), top_value / len(split)))
        loudness = loudness * jnp.repeat(draws, extent[dim] // shards_of).reshape([-1 if axis == dim else 1 for axis in range(len(extent))])
    return loudness


def noise(own_key, extent, width, bound, split=(), held_as=jnp.bfloat16):
    array = jax.random.normal(own_key, extent, jnp.float32) * width
    if len(split) > 0:
        array = shard_levels(own_key, extent, split, -0.22, 0.18) * array
    return jnp.clip(array, min=-bound, max=bound).astype(held_as)


def setup_inputs(seed: int = 0, part: int = 0) -> dict:
    seeds = jax.random.split(jax.random.key(seed), 8)
    part_splits = jax.random.split(jax.random.fold_in(seeds[7], part), 8)
    return {
        "state": noise(part_splits[0], (NS, BLK, P_SIZE, NR), 1.0, 6.0, ((0, 4), (3, 2))),
        "left_env": noise(part_splits[1], (W, NS, BLK, BLK), BLK ** -0.5, 0.375, ((1, 4),)),
        "mpo_terms": noise(seeds[2], (W, W, P_SIZE, P_SIZE), (W * P_SIZE) ** -0.5, 0.75, ((1, 2),)),
        "right_env": noise(part_splits[3], (W, NR, RB), (W * RB) ** -0.5, 0.09375, ((0, 2), (1, 2))),
        "term_charge": draw_term_charge(jax.random.fold_in(seeds[7], 71), part),
        "charge_order": draw_charge_order(jax.random.fold_in(jax.random.fold_in(seeds[7], part), 71), part),
        "sector_dims": with_ends(jax.random.randint(part_splits[6], (NS,), BLK // 2, BLK + 1), jax.random.fold_in(part_splits[6], 1), BLK // 2, BLK).astype(jnp.int32),
    }


def source_table(charge_order, first_sector, sector_count):
    own_charge = lax.dynamic_slice_in_dim(charge_order, first_sector, sector_count, 0)
    wanted = own_charge[:, None] + jnp.arange(3, dtype=jnp.int32)[None, :] - 1
    matches = charge_order[None, None, :] == wanted[:, :, None]
    sector_ids = jnp.arange(charge_order.shape[0], dtype=jnp.int32)
    found_ids = jnp.sum(jnp.where(matches, sector_ids[None, None, :], 0), axis=2).astype(jnp.int32)
    return jnp.where(jnp.any(matches, axis=2), found_ids, -1).astype(jnp.int32)


def reference(state, left_env, mpo_terms, right_env, term_charge, charge_order, sector_dims):
    sector_count = charge_order.shape[0]
    sources = source_table(charge_order, 0, sector_count)
    term_count = right_env.shape[0]
    tile_width = right_env.shape[2]
    tile_count = right_env.shape[1] // tile_width
    right_tiles = right_env.astype(jnp.float32).reshape(term_count, tile_count, tile_width, tile_width)
    mpo_float = mpo_terms.astype(jnp.float32)
    row_count = state.shape[1]
    phys = state.shape[2]
    rows_iota = jnp.arange(row_count, dtype=jnp.int32)

    def one_sector(sector):
        sector_src = sources[sector]
        safe_src = jnp.clip(sector_src, 0, sector_count - 1).astype(jnp.int32)
        blocks = state[safe_src].astype(jnp.float32) * (sector_src >= 0).astype(jnp.float32)[:, None, None, None]
        chosen = blocks[term_charge]
        environment = left_env[:, sector].astype(jnp.float32)
        applied = jnp.einsum('wxa,wapb->wxpb', environment, chosen).astype(jnp.bfloat16)
        mixed_terms = jnp.einsum('uvpq,uxqb->vxpb', mpo_float, applied.astype(jnp.float32)).astype(jnp.bfloat16)
        mixed_terms = mixed_terms.astype(jnp.float32).reshape(term_count, row_count, phys, tile_count, tile_width)
        tile_total = jnp.einsum('vxptb,vtbc->xptc', mixed_terms, right_tiles)
        tile_total = tile_total.reshape(row_count, phys, tile_count * tile_width)
        row_mask = (rows_iota < sector_dims[sector]).astype(jnp.float32)
        return (tile_total * row_mask[:, None, None]).astype(jnp.bfloat16)

    return lax.map(one_sector, jnp.arange(sector_count, dtype=jnp.int32))
```

```python
import functools

import jax
import jax.numpy as jnp
from jax import lax
from jax.experimental import pallas as pl
from jax.experimental.pallas import tpu as pltpu
from jax.sharding import PartitionSpec as P

MESH = pl.DeviceIdType.MESH
TILE = 16
LANE = 128
SUB = 2


def kernel(
    n,
    phys,
    term_charge,
    charge_order,
    sector_dims,
    s_ref,
    m_ref,
    left_hbm,
    right_hbm,
    out_ref,
    g,
    left,
    right,
    m_all,
    big,
    arranged,
    mixed,
    total,
    send_sem,
    recv_sem,
    pass_send,
    pass_recv,
    misc_sem,
    keep_sem,
):
    i = lax.axis_index("gx")
    z = lax.axis_index("gz")
    other = 1 - z
    terms = left.shape[0]
    rows = left.shape[1]
    blocks = s_ref.shape[0]
    half = rows // 2
    piece = half // SUB
    own_terms = right_hbm.shape[0]
    own_phys = phys // 2
    has_up, has_down = i < n - 1, i > 0

    load_left = pltpu.make_async_copy(left_hbm, left, misc_sem.at[0])
    load_left.start()
    load_right = pltpu.make_async_copy(
        right_hbm, right.at[pl.ds(z * own_terms, own_terms)], misc_sem.at[1]
    )
    load_right.start()
    keep_m = pltpu.make_async_copy(m_ref, m_all.at[z], misc_sem.at[2])
    keep_m.start()
    keep_s = [
        pltpu.make_async_copy(s_ref.at[block], g[block].at[i], keep_sem.at[block])
        for block in range(blocks)
    ]
    for copy in keep_s:
        copy.start()

    barrier = pltpu.get_barrier_semaphore()

    @pl.when(has_up)
    def _():
        pl.semaphore_signal(barrier, inc=1, device_id={"gx": i + 1}, device_id_type=MESH)

    @pl.when(has_down)
    def _():
        pl.semaphore_signal(barrier, inc=1, device_id={"gx": i - 1}, device_id_type=MESH)

    pl.semaphore_signal(barrier, inc=1, device_id={"gz": other}, device_id_type=MESH)
    pl.semaphore_wait(barrier, 1 + has_up.astype(jnp.int32) + has_down.astype(jnp.int32))

    def span(sub):
        return pl.ds(pl.multiple_of(z * half + sub * piece, piece), piece)

    def hop(way, step, block, sub):
        source = i - step if way == 0 else i + step
        target = i + 1 if way == 0 else i - 1
        held = g[block].at[source, span(sub)]
        origin = s_ref.at[block, span(sub)] if step == 0 else held
        return pltpu.make_async_remote_copy(
            src_ref=origin,
            dst_ref=held,
            send_sem=send_sem.at[way, step, block, sub],
            recv_sem=recv_sem.at[way, step, block, sub],
            device_id={"gx": target},
            device_id_type=MESH,
        )

    def sends(way, step):
        if way == 0:
            return jnp.logical_and(has_up, i >= step)
        return jnp.logical_and(has_down, i + step <= n - 1)

    def receives(way, step):
        return i >= step + 1 if way == 0 else i + step + 1 <= n - 1

    def arrived(way, step, block, sub):
        source = i - 1 - step if way == 0 else i + 1 + step
        held = g[block].at[source, span(sub)]
        return pltpu.make_async_remote_copy(
            src_ref=held,
            dst_ref=held,
            send_sem=send_sem.at[way, step, block, sub],
            recv_sem=recv_sem.at[way, step, block, sub],
            device_id={"gx": i},
            device_id_type=MESH,
        )

    def across(way, step, block, sub, mine):
        source = i - 1 - step if way == 0 else i + 1 + step
        core = z if mine else other
        held = g[block].at[
            source, pl.ds(pl.multiple_of(core * half + sub * piece, piece), piece)
        ]
        return pltpu.make_async_remote_copy(
            src_ref=held,
            dst_ref=held,
            send_sem=pass_send.at[way, step, block, sub],
            recv_sem=pass_recv.at[way, step, block, sub],
            device_id={"gz": other},
            device_id_type=MESH,
        )

    def start_own(block):
        for sub in range(SUB):
            for way in (0, 1):

                @pl.when(sends(way, 0))
                def _():
                    hop(way, 0, block, sub).start()

    def event(block, step):
        for sub in range(SUB):
            for way in (0, 1):

                @pl.when(receives(way, step))
                def _():
                    arrived(way, step, block, sub).wait_recv()
                    if step + 1 < n - 1:

                        @pl.when(sends(way, step + 1))
                        def _():
                            hop(way, step + 1, block, sub).start()

                    across(way, step, block, sub, True).start()

    def finish(block):
        for step in range(n - 1):
            for sub in range(SUB):
                for way in (0, 1):

                    @pl.when(receives(way, step))
                    def _():
                        across(way, step, block, sub, False).wait_recv()

    start_own(0)
    give_m = pltpu.make_async_remote_copy(
        src_ref=m_ref,
        dst_ref=m_all.at[z],
        send_sem=misc_sem.at[4],
        recv_sem=misc_sem.at[5],
        device_id={"gz": other},
        device_id_type=MESH,
    )
    give_m.start()
    give_right = pltpu.make_async_remote_copy(
        src_ref=right_hbm,
        dst_ref=right.at[pl.ds(z * own_terms, own_terms)],
        send_sem=misc_sem.at[6],
        recv_sem=misc_sem.at[7],
        device_id={"gz": other},
        device_id_type=MESH,
    )
    give_right.start()

    for held in g:
        held[n] = jnp.zeros(held.shape[1:], held.dtype)

    keep_m.wait()
    give_m.wait()
    out_rows, in_rows = big.shape
    pairs = m_all.shape[1]
    r = lax.broadcasted_iota(jnp.int32, (out_rows, 2 * pairs), 0) // TILE
    k = lax.broadcasted_iota(jnp.int32, (out_rows, 2 * pairs), 1)
    v = r % terms
    p = r // terms + z * own_phys
    wanted = (v // own_terms) * pairs + p * own_terms + v % own_terms
    pick = (k == wanted).astype(jnp.bfloat16)
    coeffs = jnp.dot(
        pick,
        m_all[...].reshape(2 * pairs, m_all.shape[2]),
        preferred_element_type=jnp.float32,
    ).astype(jnp.bfloat16)
    width = m_all.shape[2]
    spread = (
        lax.broadcasted_iota(jnp.int32, (width, in_rows), 0)
        == lax.broadcasted_iota(jnp.int32, (width, in_rows), 1) // TILE
    ).astype(jnp.bfloat16)
    diagonal = (
        lax.broadcasted_iota(jnp.int32, (out_rows, in_rows), 0) % TILE
        == lax.broadcasted_iota(jnp.int32, (out_rows, in_rows), 1) % TILE
    )
    dense = jnp.dot(coeffs, spread, preferred_element_type=jnp.float32)
    big[...] = jnp.where(diagonal, dense, 0.0).astype(jnp.bfloat16)

    own_charge = charge_order[i]
    found = []
    for shift in range(3):
        place = jnp.int32(n)
        for sector in range(n):
            place = jnp.where(charge_order[sector] == own_charge + shift - 1, sector, place)
        found.append(place)

    def apply_left(block):
        def one_term(w, carry):
            charge = term_charge[w]
            source = jnp.where(charge == 0, found[0], jnp.where(charge == 1, found[1], found[2]))
            product = jnp.dot(
                left[w], g[block][source], preferred_element_type=jnp.float32
            ).astype(jnp.bfloat16)
            for group in range(rows // TILE):
                for q in range(phys):
                    at = pl.multiple_of(w * (phys * TILE) + q * TILE, TILE)
                    side = (group % 2) * LANE
                    arranged[group // 2, pl.ds(at, TILE), side : side + LANE] = product[
                        group * TILE : (group + 1) * TILE, q * LANE : (q + 1) * LANE
                    ]
            return carry

        lax.fori_loop(0, terms, one_term, 0)

    def mix():
        def one_pair(pair, carry):
            product = jnp.dot(
                big[...], arranged[pair], preferred_element_type=jnp.float32
            ).astype(jnp.bfloat16)
            for p in range(own_phys):
                for v in range(terms):
                    for side in range(2):
                        at = pl.multiple_of(p * rows + pair * 2 * TILE + side * TILE, TILE)
                        start = (p * terms + v) * TILE
                        mixed[pl.ds(at, TILE), v * LANE : (v + 1) * LANE] = product[
                            start : start + TILE, side * LANE : (side + 1) * LANE
                        ]
            return carry

        lax.fori_loop(0, arranged.shape[0], one_pair, 0)

    def apply_right(block):
        tiles = right[:, block * LANE : (block + 1) * LANE, :].reshape(
            terms * LANE, right.shape[2]
        )
        for p in range(own_phys):
            part = slice(p * rows, (p + 1) * rows)
            product = jnp.dot(mixed[part, :], tiles, preferred_element_type=jnp.float32)
            if block == 0:
                total[part, :] = product
            else:
                total[part, :] += product

    for step in range(n - 1):
        event(0, step)
    load_left.wait()
    for copy in keep_s:
        copy.wait()
    for block in range(blocks):
        more = block + 1 < blocks
        if more:
            start_own(block + 1)
        finish(block)
        apply_left(block)
        if more:
            event(block + 1, 0)
        mix()
        if block == 0:
            load_right.wait()
            give_right.wait()
        if more and n > 2:
            event(block + 1, 1)
        apply_right(block)
        if more:
            for step in range(2, n - 1):
                event(block + 1, step)

    used = sector_dims[i]
    mask = lax.broadcasted_iota(jnp.int32, (rows, total.shape[1]), 0) < used
    for p in range(own_phys):
        out_ref[p] = jnp.where(mask, total[p * rows : (p + 1) * rows, :], 0.0).astype(
            out_ref.dtype
        )

    for block in range(blocks):
        for step in range(n - 1):
            for sub in range(SUB):
                for way in (0, 1):

                    @pl.when(sends(way, step))
                    def _():
                        hop(way, step, block, sub).wait_send()

                    @pl.when(receives(way, step))
                    def _():
                        across(way, step, block, sub, True).wait_send()


def body(n, state, left_env, mpo_terms, right_env, term_charge, charge_order, sector_dims):
    _, rows, phys, cols = state.shape
    terms, own_terms = mpo_terms.shape[:2]
    blocks = cols // LANE
    own_phys = phys // 2
    arranged_state = (
        state.reshape(rows, phys, blocks, LANE)
        .transpose(2, 0, 1, 3)
        .reshape(blocks, rows, phys * LANE)
    )
    m_own = mpo_terms.transpose(2, 1, 0, 3).reshape(phys * own_terms, terms * phys)
    m_own = jnp.pad(m_own, ((0, 0), (0, -(terms * phys) % LANE)))
    smem = pl.BlockSpec(memory_space=pltpu.SMEM)
    vmem = pl.BlockSpec(memory_space=pltpu.VMEM)
    hbm = pl.BlockSpec(memory_space=pl.ANY)
    dma = pltpu.SemaphoreType.DMA
    steps = (2, n - 1, blocks, SUB)
    out = pl.pallas_call(
        functools.partial(kernel, n, phys),
        out_shape=jax.ShapeDtypeStruct((own_phys, rows, cols), jnp.bfloat16),
        in_specs=[smem, smem, smem, vmem, vmem, hbm, hbm],
        out_specs=vmem,
        scratch_shapes=[
            [pltpu.VMEM((n + 1, rows, phys * LANE), jnp.bfloat16) for _ in range(blocks)],
            pltpu.VMEM((terms, rows, rows), jnp.bfloat16),
            pltpu.VMEM((terms, cols, cols), jnp.bfloat16),
            pltpu.VMEM((2,) + m_own.shape, jnp.bfloat16),
            pltpu.VMEM((own_phys * terms * TILE, terms * phys * TILE), jnp.bfloat16),
            pltpu.VMEM((rows // TILE // 2, terms * phys * TILE, 2 * LANE), jnp.bfloat16),
            pltpu.VMEM((own_phys * rows, terms * LANE), jnp.bfloat16),
            pltpu.VMEM((own_phys * rows, cols), jnp.float32),
            dma(steps),
            dma(steps),
            dma(steps),
            dma(steps),
            dma((8,)),
            dma((blocks,)),
        ],
        compiler_params=pltpu.CompilerParams(
            collective_id=0, has_side_effects=True, vmem_limit_bytes=56 * 1024 * 1024
        ),
        name="two_site",
    )(
        term_charge,
        charge_order,
        sector_dims,
        arranged_state,
        m_own,
        left_env.reshape(left_env.shape[0], rows, rows),
        right_env,
    )
    return out.transpose(1, 0, 2)[None]


def solution(mesh):
    return jax.shard_map(
        functools.partial(body, mesh.shape["gx"]),
        mesh=mesh,
        in_specs=(
            P(("ga", "gx"), None, None, "gy"),
            P(None, ("ga", "gx"), None, None),
            P(None, "gz", None, None),
            P("gz", ("ga", "gy"), None),
            P(),
            P("ga"),
            P("ga"),
        ),
        out_specs=P(("ga", "gx"), None, "gz", "gy"),
        check_vma=False,
    )
```

```python
import functools

import jax
import jax.numpy as jnp
from jax import lax
from jax.experimental import pallas as pl
from jax.experimental.pallas import tpu as pltpu
from jax.sharding import PartitionSpec as P

MESH = pl.DeviceIdType.MESH
TILE = 16
LANE = 128
SUB = 2


def kernel(
    n,
    phys,
    term_charge,
    charge_order,
    sector_dims,
    s_ref,
    m_ref,
    left_hbm,
    right_hbm,
    out_ref,
    g,
    left,
    right,
    m_all,
    big,
    arranged,
    mixed,
    total,
    send_sem,
    recv_sem,
    pass_send,
    pass_recv,
    misc_sem,
    keep_sem,
):
    i = lax.axis_index("gx")
    z = lax.axis_index("gz")
    other = 1 - z
    terms = left.shape[0]
    rows = left.shape[1]
    blocks = len(g)
    half = rows // 2
    piece = half // SUB
    own_terms = right_hbm.shape[0]
    own_phys = phys // 2
    has_up, has_down = i < n - 1, i > 0

    load_left = pltpu.make_async_copy(left_hbm, left, misc_sem.at[0])
    load_left.start()
    load_right = pltpu.make_async_copy(
        right_hbm, right.at[pl.ds(z * own_terms, own_terms)], misc_sem.at[1]
    )
    load_right.start()
    keep_m = pltpu.make_async_copy(m_ref, m_all.at[z], misc_sem.at[2])
    keep_m.start()
    keep_s = [
        pltpu.make_async_copy(
            s_ref.at[:, :, block * LANE : (block + 1) * LANE],
            g[block].at[i],
            keep_sem.at[block],
        )
        for block in range(blocks)
    ]
    for copy in keep_s:
        copy.start()

    barrier = pltpu.get_barrier_semaphore()

    @pl.when(has_up)
    def _():
        pl.semaphore_signal(barrier, inc=1, device_id={"gx": i + 1}, device_id_type=MESH)

    @pl.when(has_down)
    def _():
        pl.semaphore_signal(barrier, inc=1, device_id={"gx": i - 1}, device_id_type=MESH)

    pl.semaphore_signal(barrier, inc=1, device_id={"gz": other}, device_id_type=MESH)
    pl.semaphore_wait(barrier, 1 + has_up.astype(jnp.int32) + has_down.astype(jnp.int32))

    def span(sub):
        return pl.ds(pl.multiple_of(z * half + sub * piece, piece), piece)

    def hop(way, step, block, sub):
        source = i - step if way == 0 else i + step
        target = i + 1 if way == 0 else i - 1
        held = g[block].at[source, :, span(sub)]
        origin = s_ref.at[:, span(sub), block * LANE : (block + 1) * LANE] if step == 0 else held
        return pltpu.make_async_remote_copy(
            src_ref=origin,
            dst_ref=held,
            send_sem=send_sem.at[way, step, block, sub],
            recv_sem=recv_sem.at[way, step, block, sub],
            device_id={"gx": target},
            device_id_type=MESH,
        )

    def sends(way, step):
        if way == 0:
            return jnp.logical_and(has_up, i >= step)
        return jnp.logical_and(has_down, i + step <= n - 1)

    def receives(way, step):
        return i >= step + 1 if way == 0 else i + step + 1 <= n - 1

    def arrived(way, step, block, sub):
        source = i - 1 - step if way == 0 else i + 1 + step
        held = g[block].at[source, :, span(sub)]
        return pltpu.make_async_remote_copy(
            src_ref=held,
            dst_ref=held,
            send_sem=send_sem.at[way, step, block, sub],
            recv_sem=recv_sem.at[way, step, block, sub],
            device_id={"gx": i},
            device_id_type=MESH,
        )

    def across(way, step, block, sub, mine):
        source = i - 1 - step if way == 0 else i + 1 + step
        core = z if mine else other
        held = g[block].at[
            source, :, pl.ds(pl.multiple_of(core * half + sub * piece, piece), piece)
        ]
        return pltpu.make_async_remote_copy(
            src_ref=held,
            dst_ref=held,
            send_sem=pass_send.at[way, step, block, sub],
            recv_sem=pass_recv.at[way, step, block, sub],
            device_id={"gz": other},
            device_id_type=MESH,
        )

    def start_own(block):
        for sub in range(SUB):
            for way in (0, 1):

                @pl.when(sends(way, 0))
                def _():
                    hop(way, 0, block, sub).start()

    def event(block, step):
        for sub in range(SUB):
            for way in (0, 1):

                @pl.when(receives(way, step))
                def _():
                    arrived(way, step, block, sub).wait_recv()
                    if step + 1 < n - 1:

                        @pl.when(sends(way, step + 1))
                        def _():
                            hop(way, step + 1, block, sub).start()

                    across(way, step, block, sub, True).start()

    def finish(block):
        for step in range(n - 1):
            for sub in range(SUB):
                for way in (0, 1):

                    @pl.when(receives(way, step))
                    def _():
                        across(way, step, block, sub, False).wait_recv()

    start_own(0)
    give_m = pltpu.make_async_remote_copy(
        src_ref=m_ref,
        dst_ref=m_all.at[z],
        send_sem=misc_sem.at[4],
        recv_sem=misc_sem.at[5],
        device_id={"gz": other},
        device_id_type=MESH,
    )
    give_m.start()
    give_right = pltpu.make_async_remote_copy(
        src_ref=right_hbm,
        dst_ref=right.at[pl.ds(z * own_terms, own_terms)],
        send_sem=misc_sem.at[6],
        recv_sem=misc_sem.at[7],
        device_id={"gz": other},
        device_id_type=MESH,
    )
    give_right.start()

    for held in g:
        held[n] = jnp.zeros(held.shape[1:], held.dtype)

    keep_m.wait()
    give_m.wait()
    out_rows, in_rows = big.shape
    pairs = m_all.shape[1]
    kept = own_phys * terms
    r = lax.broadcasted_iota(jnp.int32, (kept, 2 * pairs), 0)
    k = lax.broadcasted_iota(jnp.int32, (kept, 2 * pairs), 1)
    v = r % terms
    p = r // terms + z * own_phys
    wanted = (v // own_terms) * pairs + p * own_terms + v % own_terms
    pick = (k == wanted).astype(jnp.bfloat16)
    coeffs = jnp.dot(
        pick,
        m_all[...].reshape(2 * pairs, m_all.shape[2]),
        preferred_element_type=jnp.float32,
    ).astype(jnp.bfloat16)
    width = m_all.shape[2]
    spread = (
        lax.broadcasted_iota(jnp.int32, (width, in_rows), 0)
        == lax.broadcasted_iota(jnp.int32, (width, in_rows), 1) // TILE
    ).astype(jnp.bfloat16)
    diagonal = (
        lax.broadcasted_iota(jnp.int32, (TILE, in_rows), 0)
        == lax.broadcasted_iota(jnp.int32, (TILE, in_rows), 1) % TILE
    )
    dense = jnp.dot(coeffs, spread, preferred_element_type=jnp.float32)
    for row in range(kept):
        big[row * TILE : (row + 1) * TILE, :] = jnp.where(
            diagonal, dense[row : row + 1, :], 0.0
        ).astype(jnp.bfloat16)

    own_charge = charge_order[i]
    found = []
    for shift in range(3):
        place = jnp.int32(n)
        for sector in range(n):
            place = jnp.where(charge_order[sector] == own_charge + shift - 1, sector, place)
        found.append(place)

    def apply_left(block):
        def one_term(w, carry):
            charge = term_charge[w]
            source = jnp.where(charge == 0, found[0], jnp.where(charge == 1, found[1], found[2]))
            taken = g[block][source]
            product = jnp.dot(
                left[w],
                jnp.concatenate([taken[q] for q in range(phys)], axis=1),
                preferred_element_type=jnp.float32,
            ).astype(jnp.bfloat16)
            for group in range(rows // TILE):
                for q in range(phys):
                    at = pl.multiple_of(w * (phys * TILE) + q * TILE, TILE)
                    side = (group % 2) * LANE
                    arranged[group // 2, pl.ds(at, TILE), side : side + LANE] = product[
                        group * TILE : (group + 1) * TILE, q * LANE : (q + 1) * LANE
                    ]
            return carry

        lax.fori_loop(0, terms, one_term, 0, unroll=8)

    def mix():
        def one_pair(pair, carry):
            product = jnp.dot(
                big[...], arranged[pair], preferred_element_type=jnp.float32
            ).astype(jnp.bfloat16)
            for p in range(own_phys):
                for v in range(terms):
                    for side in range(2):
                        at = pl.multiple_of(p * rows + pair * 2 * TILE + side * TILE, TILE)
                        start = (p * terms + v) * TILE
                        mixed[pl.ds(at, TILE), v * LANE : (v + 1) * LANE] = product[
                            start : start + TILE, side * LANE : (side + 1) * LANE
                        ]
            return carry

        lax.fori_loop(0, arranged.shape[0], one_pair, 0, unroll=4)

    def apply_right(block):
        tiles = right[:, block * LANE : (block + 1) * LANE, :].reshape(
            terms * LANE, right.shape[2]
        )
        for p in range(own_phys):
            part = slice(p * rows, (p + 1) * rows)
            product = jnp.dot(mixed[part, :], tiles, preferred_element_type=jnp.float32)
            if block == 0:
                total[part, :] = product
            else:
                total[part, :] += product

    for step in range(n - 1):
        event(0, step)
    load_left.wait()
    for copy in keep_s:
        copy.wait()
    for block in range(blocks):
        more = block + 1 < blocks
        if more:
            start_own(block + 1)
        finish(block)
        apply_left(block)
        if more:
            event(block + 1, 0)
        mix()
        if block == 0:
            load_right.wait()
            give_right.wait()
        if more and n > 2:
            event(block + 1, 1)
        apply_right(block)
        if more:
            for step in range(2, n - 1):
                event(block + 1, step)

    used = sector_dims[i]
    mask = lax.broadcasted_iota(jnp.int32, (rows, total.shape[1]), 0) < used
    for p in range(own_phys):
        out_ref[p] = jnp.where(mask, total[p * rows : (p + 1) * rows, :], 0.0).astype(
            out_ref.dtype
        )

    for block in range(blocks):
        for step in range(n - 1):
            for sub in range(SUB):
                for way in (0, 1):

                    @pl.when(sends(way, step))
                    def _():
                        hop(way, step, block, sub).wait_send()

                    @pl.when(receives(way, step))
                    def _():
                        across(way, step, block, sub, True).wait_send()


def body(n, state, left_env, mpo_terms, right_env, term_charge, charge_order, sector_dims):
    _, rows, phys, cols = state.shape
    terms, own_terms = mpo_terms.shape[:2]
    blocks = cols // LANE
    own_phys = phys // 2
    arranged_state = state.reshape(rows, phys, cols).transpose(1, 0, 2)
    m_own = mpo_terms.transpose(2, 1, 0, 3).reshape(phys * own_terms, terms * phys)
    smem = pl.BlockSpec(memory_space=pltpu.SMEM)
    vmem = pl.BlockSpec(memory_space=pltpu.VMEM)
    hbm = pl.BlockSpec(memory_space=pl.ANY)
    dma = pltpu.SemaphoreType.DMA
    steps = (2, n - 1, blocks, SUB)
    out = pl.pallas_call(
        functools.partial(kernel, n, phys),
        out_shape=jax.ShapeDtypeStruct((own_phys, rows, cols), jnp.bfloat16),
        in_specs=[smem, smem, smem, vmem, vmem, hbm, hbm],
        out_specs=vmem,
        scratch_shapes=[
            [pltpu.VMEM((n + 1, phys, rows, LANE), jnp.bfloat16) for _ in range(blocks)],
            pltpu.VMEM((terms, rows, rows), jnp.bfloat16),
            pltpu.VMEM((terms, cols, cols), jnp.bfloat16),
            pltpu.VMEM((2,) + m_own.shape, jnp.bfloat16),
            pltpu.VMEM((own_phys * terms * TILE, terms * phys * TILE), jnp.bfloat16),
            pltpu.VMEM((rows // TILE // 2, terms * phys * TILE, 2 * LANE), jnp.bfloat16),
            pltpu.VMEM((own_phys * rows, terms * LANE), jnp.bfloat16),
            pltpu.VMEM((own_phys * rows, cols), jnp.float32),
            dma(steps),
            dma(steps),
            dma(steps),
            dma(steps),
            dma((8,)),
            dma((blocks,)),
        ],
        compiler_params=pltpu.CompilerParams(
            collective_id=0, has_side_effects=True, vmem_limit_bytes=56 * 1024 * 1024
        ),
        name="two_site",
    )(
        term_charge,
        charge_order,
        sector_dims,
        arranged_state,
        m_own,
        left_env.reshape(left_env.shape[0], rows, rows),
        right_env,
    )
    return out.transpose(1, 0, 2)[None]


def solution(mesh):
    return jax.shard_map(
        functools.partial(body, mesh.shape["gx"]),
        mesh=mesh,
        in_specs=(
            P(("ga", "gx"), None, None, "gy"),
            P(None, ("ga", "gx"), None, None),
            P(None, "gz", None, None),
            P("gz", ("ga", "gy"), None),
            P(),
            P("ga"),
            P("ga"),
        ),
        out_specs=P(("ga", "gx"), None, "gz", "gy"),
        check_vma=False,
    )
```

```python
import functools

import jax
import jax.numpy as jnp
from jax import lax
from jax.experimental import pallas as pl
from jax.experimental.pallas import tpu as pltpu
from jax.sharding import PartitionSpec as P

MESH = pl.DeviceIdType.MESH
TILE = 16
LANE = 128
SUB = 2


def kernel(
    n,
    phys,
    term_charge,
    charge_order,
    sector_dims,
    s_ref,
    m_ref,
    left_hbm,
    right_hbm,
    out_ref,
    g,
    left,
    right,
    m_all,
    coeffs,
    big,
    arranged,
    mixed,
    total,
    send_sem,
    recv_sem,
    pass_send,
    pass_recv,
    misc_sem,
    keep_sem,
    stage,
    pick_send,
    pick_recv,
    pick_pass_send,
    pick_pass_recv,
):
    i = lax.axis_index("gx")
    z = lax.axis_index("gz")
    other = 1 - z
    terms = left.shape[0]
    rows = left.shape[1]
    blocks = len(g)
    half = rows // 2
    piece = half // SUB
    own_terms = right_hbm.shape[0]
    own_phys = phys // 2
    has_up, has_down = i < n - 1, i > 0

    load_left = pltpu.make_async_copy(left_hbm, left, misc_sem.at[0])
    load_left.start()
    load_right = pltpu.make_async_copy(
        right_hbm, right.at[pl.ds(z * own_terms, own_terms)], misc_sem.at[1]
    )
    load_right.start()
    keep_m = pltpu.make_async_copy(m_ref, m_all.at[z], misc_sem.at[2])
    keep_m.start()
    keep_s = [
        pltpu.make_async_copy(
            s_ref.at[:, :, block * LANE : (block + 1) * LANE],
            g[block].at[i],
            keep_sem.at[block],
        )
        for block in range(blocks)
    ]
    for copy in keep_s:
        copy.start()

    barrier = pltpu.get_barrier_semaphore()

    @pl.when(has_up)
    def _():
        pl.semaphore_signal(barrier, inc=1, device_id={"gx": i + 1}, device_id_type=MESH)

    @pl.when(has_down)
    def _():
        pl.semaphore_signal(barrier, inc=1, device_id={"gx": i - 1}, device_id_type=MESH)

    pl.semaphore_signal(barrier, inc=1, device_id={"gz": other}, device_id_type=MESH)
    pl.semaphore_wait(barrier, 1 + has_up.astype(jnp.int32) + has_down.astype(jnp.int32))

    def span(sub):
        return pl.ds(pl.multiple_of(z * half + sub * piece, piece), piece)

    def hop(way, step, block, sub):
        source = i - step if way == 0 else i + step
        target = i + 1 if way == 0 else i - 1
        held = g[block].at[source, :, span(sub)]
        origin = s_ref.at[:, span(sub), block * LANE : (block + 1) * LANE] if step == 0 else held
        return pltpu.make_async_remote_copy(
            src_ref=origin,
            dst_ref=held,
            send_sem=send_sem.at[way, step, block, sub],
            recv_sem=recv_sem.at[way, step, block, sub],
            device_id={"gx": target},
            device_id_type=MESH,
        )

    picky = 1 if n >= 4 else 0

    def sends(way, step):
        if way == 0:
            return jnp.logical_and(i < n - 1 - picky, i >= step)
        return jnp.logical_and(i > picky, i + step <= n - 1)

    def receives(way, step):
        if way == 0:
            return jnp.logical_and(i >= step + 1, i <= n - 1 - picky)
        return jnp.logical_and(i + step + 1 <= n - 1, i >= picky)

    def arrived(way, step, block, sub):
        source = i - 1 - step if way == 0 else i + 1 + step
        held = g[block].at[source, :, span(sub)]
        return pltpu.make_async_remote_copy(
            src_ref=held,
            dst_ref=held,
            send_sem=send_sem.at[way, step, block, sub],
            recv_sem=recv_sem.at[way, step, block, sub],
            device_id={"gx": i},
            device_id_type=MESH,
        )

    def across(way, step, block, sub, mine):
        source = i - 1 - step if way == 0 else i + 1 + step
        core = z if mine else other
        held = g[block].at[
            source, :, pl.ds(pl.multiple_of(core * half + sub * piece, piece), piece)
        ]
        return pltpu.make_async_remote_copy(
            src_ref=held,
            dst_ref=held,
            send_sem=pass_send.at[way, step, block, sub],
            recv_sem=pass_recv.at[way, step, block, sub],
            device_id={"gz": other},
            device_id_type=MESH,
        )

    def find(sector_charge, shift):
        place = jnp.int32(n)
        for sector in range(n):
            place = jnp.where(charge_order[sector] == sector_charge + shift - 1, sector, place)
        return place

    def choice(way):
        end_charge = charge_order[n - 1 if way == 0 else 0]
        first, second = find(end_charge, 0), find(end_charge, 2)
        if way == 0:
            first = jnp.where(first < n, n - 1 - first, n)
            second = jnp.where(second < n, n - 1 - second, n)
        near, far = jnp.minimum(first, second), jnp.maximum(first, second)
        return (
            jnp.where(near < n - 1, near, 1),
            jnp.where(far < n, far, near),
            first,
            second,
        )

    found = [find(charge_order[i], shift) for shift in range(3)]
    choices = [choice(way) for way in (0, 1)] if picky else []
    for way in range(len(choices)):
        early, _, first, second = choices[way]
        end = n - 1 if way == 0 else 0
        for shift, sought in ((0, first), (2, second)):
            one, two = (n - 2, n - 3) if way == 0 else (1, 2)
            place = jnp.where(sought == n, n, jnp.where(sought == early, one, two))
            found[shift] = jnp.where(i == end, place, found[shift])

    half_rows = pl.ds(pl.multiple_of(z * half, half), half)
    other_rows = pl.ds(pl.multiple_of(other * half, half), half)

    def picked(way, which, block, passing, mine=True):
        slot = (n - 2 - which) if way == 0 else 1 + which
        held = g[block].at[slot, :, half_rows if mine else other_rows]
        return pltpu.make_async_remote_copy(
            src_ref=held if passing else stage.at[which, block],
            dst_ref=held,
            send_sem=(pick_pass_send if passing else pick_send).at[way, which, block],
            recv_sem=(pick_pass_recv if passing else pick_recv).at[way, which, block],
            device_id={"gz": other} if passing else {"gx": n - 1 if way == 0 else 0},
            device_id_type=MESH,
        )

    def pick(block, which):
        for way in range(len(choices)):

            @pl.when(i == (n - 2 if way == 0 else 1))
            def _():
                value = s_ref[:, half_rows, block * LANE : (block + 1) * LANE]
                for place in range(2, n - 1 + which):
                    slot = n - 1 - place if way == 0 else place
                    value = jnp.where(
                        choices[way][which] == place, g[block][slot, :, half_rows], value
                    )
                stage[which, block] = value
                picked(way, which, block, False).start()

    def take(block, which):
        for way in range(len(choices)):

            @pl.when(i == (n - 1 if way == 0 else 0))
            def _():
                picked(way, which, block, False).wait_recv()
                picked(way, which, block, True).start()

    def settle():
        for block in range(blocks):
            for which in range(2):
                for way in range(len(choices)):

                    @pl.when(i == (n - 2 if way == 0 else 1))
                    def _():
                        picked(way, which, block, False).wait_send()

                    @pl.when(i == (n - 1 if way == 0 else 0))
                    def _():
                        picked(way, which, block, True).wait_send()

    def start_own(block):
        for sub in range(SUB):
            for way in (0, 1):

                @pl.when(sends(way, 0))
                def _():
                    hop(way, 0, block, sub).start()

    def event(block, step):
        for sub in range(SUB):
            for way in (0, 1):

                @pl.when(receives(way, step))
                def _():
                    arrived(way, step, block, sub).wait_recv()
                    if step + 1 < n - 1:

                        @pl.when(sends(way, step + 1))
                        def _():
                            hop(way, step + 1, block, sub).start()

                    across(way, step, block, sub, True).start()

    def flow(block, step):
        event(block, step)
        if picky and step == n - 4:
            pick(block, 0)
        if picky and step == n - 3:
            pick(block, 1)
            take(block, 0)

    def finish(block):
        for step in range(n - 1):
            for sub in range(SUB):
                for way in (0, 1):

                    @pl.when(receives(way, step))
                    def _():
                        across(way, step, block, sub, False).wait_recv()
        for way in range(len(choices)):

            @pl.when(i == (n - 1 if way == 0 else 0))
            def _():
                for which in range(2):
                    picked(way, which, block, True, False).wait_recv()

    start_own(0)
    give_m = pltpu.make_async_remote_copy(
        src_ref=m_ref,
        dst_ref=m_all.at[z],
        send_sem=misc_sem.at[4],
        recv_sem=misc_sem.at[5],
        device_id={"gz": other},
        device_id_type=MESH,
    )
    give_m.start()
    give_right = pltpu.make_async_remote_copy(
        src_ref=right_hbm,
        dst_ref=right.at[pl.ds(z * own_terms, own_terms)],
        send_sem=misc_sem.at[6],
        recv_sem=misc_sem.at[7],
        device_id={"gz": other},
        device_id_type=MESH,
    )
    give_right.start()

    for held in g:
        held[n] = jnp.zeros(held.shape[1:], held.dtype)

    keep_m.wait()
    give_m.wait()
    kept = own_phys * terms
    width = terms * TILE
    spread = (
        lax.broadcasted_iota(jnp.int32, (terms, width), 0)
        == lax.broadcasted_iota(jnp.int32, (terms, width), 1) // TILE
    ).astype(jnp.bfloat16)
    diagonal = (
        lax.broadcasted_iota(jnp.int32, (TILE, width), 0)
        == lax.broadcasted_iota(jnp.int32, (TILE, width), 1) % TILE
    )
    entries = m_all.shape[1]
    coeffs[...] = jnp.dot(
        m_all[...].reshape(2 * entries, terms), spread, preferred_element_type=jnp.float32
    )
    for row in range(kept):
        v = row % terms
        p = row // terms + z * own_phys
        for q in range(phys):
            at = (v // own_terms) * entries + ((v % own_terms) * phys + p) * phys + q
            big[row * TILE : (row + 1) * TILE, q * width : (q + 1) * width] = jnp.where(
                diagonal, coeffs[pl.ds(at, 1), :], 0.0
            ).astype(jnp.bfloat16)

    def apply_left(block):
        def one_term(w, carry):
            charge = term_charge[w]
            source = jnp.where(charge == 0, found[0], jnp.where(charge == 1, found[1], found[2]))
            taken = g[block][source]
            product = jnp.dot(
                left[w],
                jnp.concatenate([taken[q] for q in range(phys)], axis=1),
                preferred_element_type=jnp.float32,
            ).astype(jnp.bfloat16)
            for group in range(rows // TILE):
                for q in range(phys):
                    at = pl.multiple_of(w * TILE + q * (terms * TILE), TILE)
                    side = (group % 2) * LANE
                    arranged[group // 2, pl.ds(at, TILE), side : side + LANE] = product[
                        group * TILE : (group + 1) * TILE, q * LANE : (q + 1) * LANE
                    ]
            return carry

        lax.fori_loop(0, terms, one_term, 0, unroll=8)

    def mix():
        def one_pair(pair, carry):
            product = jnp.dot(
                big[...], arranged[pair], preferred_element_type=jnp.float32
            ).astype(jnp.bfloat16)
            for p in range(own_phys):
                for v in range(terms):
                    for side in range(2):
                        at = pl.multiple_of(p * rows + pair * 2 * TILE + side * TILE, TILE)
                        start = (p * terms + v) * TILE
                        mixed[pl.ds(at, TILE), v * LANE : (v + 1) * LANE] = product[
                            start : start + TILE, side * LANE : (side + 1) * LANE
                        ]
            return carry

        lax.fori_loop(0, arranged.shape[0], one_pair, 0, unroll=4)

    def apply_right(block):
        tiles = right[:, block * LANE : (block + 1) * LANE, :].reshape(
            terms * LANE, right.shape[2]
        )
        for p in range(own_phys):
            part = slice(p * rows, (p + 1) * rows)
            product = jnp.dot(mixed[part, :], tiles, preferred_element_type=jnp.float32)
            if block == 0:
                total[part, :] = product
            else:
                total[part, :] += product

    for step in range(n - 1):
        flow(0, step)
    take(0, 1)
    load_left.wait()
    for copy in keep_s:
        copy.wait()
    for block in range(blocks):
        more = block + 1 < blocks
        if more:
            start_own(block + 1)
        finish(block)
        apply_left(block)
        if more:
            flow(block + 1, 0)
        mix()
        if block == 0:
            load_right.wait()
            give_right.wait()
        if more and n > 2:
            flow(block + 1, 1)
        apply_right(block)
        if more:
            for step in range(2, n - 1):
                flow(block + 1, step)
            take(block + 1, 1)

    settle()
    used = sector_dims[i]
    mask = lax.broadcasted_iota(jnp.int32, (rows, total.shape[1]), 0) < used
    for p in range(own_phys):
        out_ref[p] = jnp.where(mask, total[p * rows : (p + 1) * rows, :], 0.0).astype(
            out_ref.dtype
        )

    for block in range(blocks):
        for step in range(n - 1):
            for sub in range(SUB):
                for way in (0, 1):

                    @pl.when(sends(way, step))
                    def _():
                        hop(way, step, block, sub).wait_send()

                    @pl.when(receives(way, step))
                    def _():
                        across(way, step, block, sub, True).wait_send()


def body(n, state, left_env, mpo_terms, right_env, term_charge, charge_order, sector_dims):
    _, rows, phys, cols = state.shape
    terms, own_terms = mpo_terms.shape[:2]
    blocks = cols // LANE
    own_phys = phys // 2
    arranged_state = state.reshape(rows, phys, cols).transpose(1, 0, 2)
    m_own = mpo_terms.transpose(1, 2, 3, 0).reshape(own_terms * phys * phys, terms)
    smem = pl.BlockSpec(memory_space=pltpu.SMEM)
    vmem = pl.BlockSpec(memory_space=pltpu.VMEM)
    hbm = pl.BlockSpec(memory_space=pl.ANY)
    dma = pltpu.SemaphoreType.DMA
    steps = (2, n - 1, blocks, SUB)
    out = pl.pallas_call(
        functools.partial(kernel, n, phys),
        out_shape=jax.ShapeDtypeStruct((own_phys, rows, cols), jnp.bfloat16),
        in_specs=[smem, smem, smem, vmem, vmem, hbm, hbm],
        out_specs=vmem,
        scratch_shapes=[
            [pltpu.VMEM((n + 1, phys, rows, LANE), jnp.bfloat16) for _ in range(blocks)],
            pltpu.VMEM((terms, rows, rows), jnp.bfloat16),
            pltpu.VMEM((terms, cols, cols), jnp.bfloat16),
            pltpu.VMEM((2,) + m_own.shape, jnp.bfloat16),
            pltpu.VMEM((2 * m_own.shape[0], terms * TILE), jnp.float32),
            pltpu.VMEM((own_phys * terms * TILE, terms * phys * TILE), jnp.bfloat16),
            pltpu.VMEM((rows // TILE // 2, terms * phys * TILE, 2 * LANE), jnp.bfloat16),
            pltpu.VMEM((own_phys * rows, terms * LANE), jnp.bfloat16),
            pltpu.VMEM((own_phys * rows, cols), jnp.float32),
            dma(steps),
            dma(steps),
            dma(steps),
            dma(steps),
            dma((8,)),
            dma((blocks,)),
            pltpu.VMEM((2, blocks, phys, rows // 2, LANE), jnp.bfloat16),
            dma((2, 2, blocks)),
            dma((2, 2, blocks)),
            dma((2, 2, blocks)),
            dma((2, 2, blocks)),
        ],
        compiler_params=pltpu.CompilerParams(
            collective_id=0, has_side_effects=True, vmem_limit_bytes=56 * 1024 * 1024
        ),
        name="two_site",
    )(
        term_charge,
        charge_order,
        sector_dims,
        arranged_state,
        m_own,
        left_env.reshape(left_env.shape[0], rows, rows),
        right_env,
    )
    return out.transpose(1, 0, 2)[None]


def solution(mesh):
    return jax.shard_map(
        functools.partial(body, mesh.shape["gx"]),
        mesh=mesh,
        in_specs=(
            P(("ga", "gx"), None, None, "gy"),
            P(None, ("ga", "gx"), None, None),
            P(None, "gz", None, None),
            P("gz", ("ga", "gy"), None),
            P(),
            P("ga"),
            P("ga"),
        ),
        out_specs=P(("ga", "gx"), None, "gz", "gy"),
        check_vma=False,
    )
```
